256 devices in a mesh: ga: 16 (over x_hi, y, core), band: 16 (over x_lo, z).
Axes of the slice: x: 4 (x_hi: 2, x_lo: 2; x = x_hi * 2 + x_lo), y: 4, z: 8, core: 2. Of those that a mesh axis runs over, the one named last changes fastest.
Arguments:
- waves: bfloat16 [2, 16384, 4096], P(None, 'ga', 'band'), may hold values from -6 to 6
- rotation: bfloat16 [2, 4096, 4096], P(None, 'ga', 'band'), may hold values from -0.0625 to 0.0625
Outputs:
- rotated: bfloat16 [2, 16384, 4096], P(None, 'ga', 'band')
The draws below stay inside these ranges and needn't reach their ends.
All inputs are finite; a program needn't handle non-finite values.
Results may differ from the reference program's by a relative error of at most 0.001.
Values may be sent and summed in bfloat16 or wider, within the bound.
A program may use at most 128 MiB of HBM per device.

```python
import jax
import jax.numpy as jnp

NB = 4096
NG = 16384


def levels(rng, shape, split, least, high):
    level, own = 1.0, jax.random.fold_in(rng, 6)
    for position, blocks in split:
        heights = jnp.exp(jax.random.uniform(jax.random.fold_in(own, position), (blocks,), jnp.float32, least / len(split), high / len(split)))
        level = level * jnp.repeat(heights, shape[position] // blocks).reshape([-1 if axis == position else 1 for axis in range(len(shape))])
    return level


def normal_values(stream_key, extent, width, reach, cuts=(), kind=jnp.bfloat16):
    drawn = jax.random.normal(stream_key, extent, jnp.float32) * width
    if len(cuts) > 0:
        drawn = levels(stream_key, extent, cuts, -0.22, 0.18) * drawn
    return jnp.clip(drawn, min=-reach, max=reach).astype(kind)


def setup_inputs(seed: int = 0) -> dict:
    arg_keys = jax.random.split(jax.random.key(seed), 3)
    waves = normal_values(arg_keys[0], (2, NG, NB), 1.0, 6.0, ((1, 16), (2, 16)))
    rotation = normal_values(arg_keys[1], (2, NB, NB), (2 * NB) ** -0.5, 0.0625, ((1, 16), (2, 16)))
    return dict(waves=waves, rotation=rotation)


def reference(waves, rotation):
    stacked = jnp.concatenate([waves[0], waves[1]], axis=1)
    real_rows = jnp.concatenate([rotation[0], rotation[1]], axis=1)
    imag_rows = jnp.concatenate([-rotation[1], rotation[0]], axis=1)
    matrix = jnp.concatenate([real_rows, imag_rows], axis=0)
    result = jnp.dot(stacked, matrix, preferred_element_type=jnp.float32)
    return jnp.stack([result[:, :NB], result[:, NB:]]).astype(jnp.bfloat16)
```

```python
import functools

import jax
import jax.numpy as jnp
from jax import lax
from jax.experimental import pallas as pl
from jax.experimental.pallas import tpu as pltpu
from jax.sharding import Mesh
from jax.sharding import PartitionSpec as P

GA = ("xh", "y", "core")
BAND = ("xl", "z")
MESH = pl.DeviceIdType.MESH

CHUNKS = (128, 128, 128, 64, 64)
STARTS = tuple(sum(CHUNKS[:i]) for i in range(len(CHUNKS)))
N = len(CHUNKS)
HALF = 512
W = 256
HOPS = ((4, 3), (3, 4))


def kernel(
    waves, rot, out,
    a, xs, b, cs, acc,
    load_sem, ax_send, ax_recv, az_send, az_recv,
    bx_send, bx_recv, by_send, by_recv, bs_send, bs_recv,
    c_send, c_recv, c_local,
):
    xh, y, core = lax.axis_index("xh"), lax.axis_index("y"), lax.axis_index("core")
    xl, z = lax.axis_index("xl"), lax.axis_index("z")
    x = xh * 2 + xl

    def at_x(dx):
        there = (x + dx + 4) % 4
        return {"xh": there // 2, "xl": there % 2}

    def at_y(dy):
        return {"y": (y + dy + 4) % 4}

    def at_z(dz):
        return {"z": (z + dz + 8) % 8}

    partner = {"xl": 1 - xl}
    sibling = {"core": 1 - core}

    def rows(i, base=0):
        return pl.ds(base + STARTS[i], CHUNKS[i])

    def piece(i, kb, dz):
        side = xl if kb == 0 else 1 - xl
        return a.at[side * 8 + (z + dz + 16) % 8, :, rows(i), :]

    def block(dx, dy, who=None):
        there = (x + dx + 4) % 4
        who = core if who is None else who
        return b.at[(there // 2) * 8 + ((y + dy + 4) % 4) * 2 + who, there % 2]

    def remote(src, dst, send, recv, where):
        return pltpu.make_async_remote_copy(
            src_ref=src, dst_ref=dst, send_sem=send, recv_sem=recv,
            device_id=where, device_id_type=MESH,
        )

    sent = []

    def go(src, dst, send, recv, where):
        copy = remote(src, dst, send, recv, where)
        copy.start()
        sent.append(copy)

    def arrived(dst, send, recv, where):
        remote(dst, dst, send, recv, where).wait_recv()

    def load_own(i):
        return pltpu.make_async_copy(
            waves.at[:, rows(i, xl * HALF), :], piece(i, 0, 0), load_sem.at[0, i])

    def load_other(i):
        return pltpu.make_async_copy(
            waves.at[:, rows(i, (1 - xl) * HALF), :], xs.at[:, rows(i), :], load_sem.at[1, i])

    load_rot = pltpu.make_async_copy(rot, block(0, 0), load_sem.at[0, N])

    load_own(0).start()
    load_other(0).start()
    load_rot.start()
    for i in range(1, N):
        load_own(i).start()
        load_other(i).start()

    barrier = pltpu.get_barrier_semaphore()
    for where in (at_x(1), at_x(-1), at_y(1), at_y(-1), at_z(1), at_z(-1), sibling):
        pl.semaphore_signal(barrier, inc=1, device_id=where, device_id_type=MESH)
    pl.semaphore_wait(barrier, 7)

    def swap(i):
        load_other(i).wait()
        go(xs.at[:, rows(i), :], piece(i, 0, 0), ax_send.at[i], ax_recv.at[i], partner)

    def slot(kb, d, t):
        return (kb * 2 + d) * 4 + t

    def ring(i, kb, d, t):
        s = slot(kb, d, t)
        ref = piece(i, kb, -t if d == 0 else t)
        go(ref, ref, az_send.at[i, s], az_recv.at[i, s], at_z(1 if d == 0 else -1))

    def own(i, kb):
        if kb == 0:
            load_own(i).wait()
        else:
            arrived(piece(i, 1, 0), ax_send.at[i], ax_recv.at[i], partner)
        ring(i, kb, 0, 0)
        ring(i, kb, 1, 0)

    def step(i, t):
        for kb in range(2):
            for d in range(2):
                if t <= HOPS[kb][d]:
                    s = slot(kb, d, t - 1)
                    arrived(piece(i, kb, -t if d == 0 else t), az_send.at[i, s],
                            az_recv.at[i, s], at_z(1 if d == 0 else -1))
                    if t < HOPS[kb][d]:
                        ring(i, kb, d, t)

    COLS = (0, -1, 1, 2)

    def to_sibling(j, k):
        ref = block(COLS[j], (0, -1, 1, 2)[k])
        go(ref, ref, bs_send.at[j, k], bs_recv.at[j, k], sibling)

    def to_y(j):
        ref = block(COLS[j], 0)
        go(ref, ref, by_send.at[j, 0], by_recv.at[j, 0], at_y(1))
        go(ref, ref, by_send.at[j, 1], by_recv.at[j, 1], at_y(-1))
        to_sibling(j, 0)

    def b_start():
        load_rot.wait()
        ref = block(0, 0)
        go(ref, ref, bx_send.at[0], bx_recv.at[0], at_x(1))
        go(ref, ref, bx_send.at[1], bx_recv.at[1], at_x(-1))
        to_y(0)

    def b_x1():
        for d, dx in ((0, -1), (1, 1)):
            ref = block(dx, 0)
            arrived(ref, bx_send.at[d], bx_recv.at[d], at_x(-dx))
            part = ref.at[d]
            go(part, part, bx_send.at[2 + d], bx_recv.at[2 + d], at_x(-dx))
            to_y(1 + d)

    def b_x2():
        for d, dx in ((0, -2), (1, 2)):
            arrived(block(2, 0).at[d], bx_send.at[2 + d], bx_recv.at[2 + d], at_x(1 - 2 * d))
        to_y(3)

    def b_y1(j):
        for d, dy in ((0, -1), (1, 1)):
            ref = block(COLS[j], dy)
            arrived(ref, by_send.at[j, d], by_recv.at[j, d], at_y(-dy))
            part = ref.at[d]
            go(part, part, by_send.at[j, 2 + d], by_recv.at[j, 2 + d], at_y(-dy))
            to_sibling(j, 1 + d)

    def b_y2(j):
        for d in range(2):
            arrived(block(COLS[j], 2).at[d], by_send.at[j, 2 + d], by_recv.at[j, 2 + d],
                    at_y(1 - 2 * d))
        to_sibling(j, 3)

    def b_sibling():
        for j in range(4):
            for k in range(4):
                arrived(block(COLS[j], (0, -1, 1, 2)[k], 1 - core),
                        bs_send.at[j, k], bs_recv.at[j, k], sibling)

    def compute(i, low, high):
        r = CHUNKS[i]
        if low == 0:
            acc[:, : 2 * r, :] = jnp.zeros((2, 2 * r, 2 * W), jnp.float32)

        def body(m, carry):
            dz = ((m + 1) // 2) * (1 - 2 * (m % 2))
            place = (z + dz + 8) % 8
            lhs = [
                a[side * 8 + place, :, rows(i), :].reshape(2 * r, W) for side in (0, 1)
            ]
            for n in range(2):
                which = 1 - xl if n == 0 else xl
                for cd in range(2):
                    total = acc[n, : 2 * r, cd * W : (cd + 1) * W]
                    for side in (0, 1):
                        total = total + jnp.dot(
                            lhs[side], b[side * 8 + place, which, cd],
                            preferred_element_type=jnp.float32)
                    acc[n, : 2 * r, cd * W : (cd + 1) * W] = total
            return carry

        lax.fori_loop(low, high, body, 0)

    def store_own(i):
        return pltpu.make_async_copy(
            cs.at[1, :, rows(i), :], out.at[:, rows(i, xl * HALF), :], c_local.at[i])

    def finish(i):
        r = CHUNKS[i]
        for n in range(2):
            cs[n, 0, rows(i), :] = (acc[n, :r, :W] - acc[n, r : 2 * r, W:]).astype(jnp.bfloat16)
            cs[n, 1, rows(i), :] = (acc[n, :r, W:] + acc[n, r : 2 * r, :W]).astype(jnp.bfloat16)
        go(cs.at[0, :, rows(i), :], out.at[:, rows(i, xl * HALF), :],
           c_send.at[i], c_recv.at[i], partner)
        store_own(i).start()

    own(0, 0)
    swap(0)
    b_start()
    swap(1)
    own(1, 0)
    own(0, 1)
    for i in range(2, N):
        swap(i)
    own(1, 1)
    step(0, 1)
    b_y1(0)
    b_x1()
    step(0, 2)
    b_x2()
    step(0, 3)
    b_y1(1)
    b_y1(2)
    own(2, 0)
    own(2, 1)
    step(1, 1)
    b_y1(3)
    step(0, 4)
    step(1, 2)
    b_y2(0)
    b_y2(1)
    b_y2(2)
    step(1, 3)
    b_y2(3)
    b_sibling()
    own(3, 0)
    own(3, 1)
    step(2, 1)
    compute(0, 0, 4)
    step(2, 2)
    compute(0, 4, 8)
    finish(0)
    step(1, 4)
    step(2, 3)
    own(4, 0)
    own(4, 1)
    compute(1, 0, 4)
    step(3, 1)
    compute(1, 4, 8)
    finish(1)
    step(3, 2)
    step(2, 4)
    compute(2, 0, 4)
    step(3, 3)
    compute(2, 4, 8)
    step(4, 1)
    finish(2)
    step(4, 2)
    step(3, 4)
    compute(3, 0, 4)
    step(4, 3)
    compute(3, 4, 8)
    finish(3)
    compute(4, 0, 7)
    step(4, 4)
    compute(4, 7, 8)
    finish(4)

    for copy in sent:
        copy.wait_send()
    for i in range(N):
        store_own(i).wait()
        arrived(out.at[:, rows(i, (1 - xl) * HALF), :], c_send.at[i], c_recv.at[i], partner)


def local(waves, rotation):
    dma = pltpu.SemaphoreType.DMA
    return pl.pallas_call(
        kernel,
        out_shape=jax.ShapeDtypeStruct(waves.shape, waves.dtype),
        in_specs=[pl.BlockSpec(memory_space=pl.ANY)] * 2,
        out_specs=pl.BlockSpec(memory_space=pl.ANY),
        scratch_shapes=[
            pltpu.VMEM((16, 2, HALF, W), jnp.bfloat16),
            pltpu.VMEM((2, HALF, W), jnp.bfloat16),
            pltpu.VMEM((16, 2, 2, W, W), jnp.bfloat16),
            pltpu.VMEM((2, 2, HALF, W), jnp.bfloat16),
            pltpu.VMEM((2, 2 * max(CHUNKS), 2 * W), jnp.float32),
            dma((2, N + 1)),
            dma((N,)), dma((N,)),
            dma((N, 16)), dma((N, 16)),
            dma((4,)), dma((4,)),
            dma((4, 4)), dma((4, 4)),
            dma((4, 4)), dma((4, 4)),
            dma((N,)), dma((N,)), dma((N,)),
        ],
        compiler_params=pltpu.CompilerParams(
            collective_id=0, has_side_effects=True, vmem_limit_bytes=60 * 1024 * 1024),
        name="rotate",
    )(waves, rotation)


def solution(mesh):
    finer = Mesh(
        mesh.devices.reshape(2, 4, 2, 2, 8), ("xh", "y", "core", "xl", "z")
    )
    return jax.shard_map(
        local,
        mesh=finer,
        in_specs=(P(None, GA, BAND), P(None, GA, BAND)),
        out_specs=P(None, GA, BAND),
        check_vma=False,
    )
```

```python
import jax
import jax.numpy as jnp
from jax import lax
from jax.experimental import pallas as pl
from jax.experimental.pallas import tpu as pltpu
from jax.sharding import Mesh
from jax.sharding import PartitionSpec as P

GA = ("xh", "y", "core")
BAND = ("xl", "z")
MESH = pl.DeviceIdType.MESH

CHUNKS = (128, 64, 64)
STARTS = tuple(sum(CHUNKS[:i]) for i in range(len(CHUNKS)))
N = len(CHUNKS)
HALF = 512
QUARTER = 256
W = 256
NEAR = (0, -1, 1, 2)


def kernel(
    waves, rot, out,
    a, u, via, xs, b, cs, acc,
    load_sem, ax_send, ax_recv, az_send, az_recv,
    bz_send, bz_recv, b1_send, b1_recv, b2_send, b2_recv, bs_send, bs_recv,
    c_send, c_recv, c_local,
):
    xh, y, core = lax.axis_index("xh"), lax.axis_index("y"), lax.axis_index("core")
    xl, z = lax.axis_index("xl"), lax.axis_index("z")
    x = xh * 2 + xl
    s = 1 - 2 * (z % 2)
    kind = (z // 2) % 2

    def plane(d):
        return (z + s * d + 8) % 8

    def at_x(dx):
        there = (x + dx + 4) % 4
        return {"xh": there // 2, "xl": there % 2}

    def at_y(dy):
        return {"y": (y + dy + 4) % 4}

    inner = {"z": plane(1)}
    outer = {"z": plane(-1)}
    partner = {"xl": 1 - xl}
    across = {"xl": 1 - xl, "z": plane(-1)}
    sibling = {"core": 1 - core}

    def rows(i, base=0):
        return pl.ds(base + STARTS[i], CHUNKS[i])

    def remote(src, dst, send, recv, where):
        return pltpu.make_async_remote_copy(
            src_ref=src, dst_ref=dst, send_sem=send, recv_sem=recv,
            device_id=where, device_id_type=MESH,
        )

    sent = []

    def go(src, dst, send, recv, where):
        copy = remote(src, dst, send, recv, where)
        copy.start()
        sent.append(copy)

    def arrived(dst, send, recv, where):
        remote(dst, dst, send, recv, where).wait_recv()

    def mine(i, kb, d):
        side = xl if kb == 0 else 1 - xl
        return a.at[side * 8 + plane(d), :, rows(i), :]

    def theirs(i, kb):
        return u.at[kb, :, rows(i), :]

    def passing(i, kb, j):
        return via.at[j, kb, :, rows(i), :]

    def spare(i, j):
        return xs.at[j, :, rows(i), :]

    def load(i, j):
        half = xl if j < 2 else 1 - xl
        quarter = kind if j % 2 == 0 else 1 - kind
        dst = (mine(i, 0, 0), theirs(i, 0), spare(i, 0), spare(i, 1))[j]
        return pltpu.make_async_copy(
            waves.at[:, rows(i, half * HALF + quarter * QUARTER), :], dst, load_sem.at[j, i])

    def swap(i):
        load(i, 2).wait()
        go(spare(i, 0), mine(i, 0, 0), ax_send.at[0, i], ax_recv.at[0, i], partner)
        load(i, 3).wait()
        go(spare(i, 1), theirs(i, 1), ax_send.at[1, i], ax_recv.at[1, i], partner)

    def landing(i, kb, n):
        if n == 1:
            return passing(i, kb, 0)
        if n == 5:
            return passing(i, kb, 1)
        if n == 6:
            return passing(i, kb, 2)
        return mine(i, kb, {0: -1, 2: -2, 3: -3, 4: 1, 7: 2, 8: 3, 9: 4}[n])

    def over(i, kb, n, src, dst):
        k = kb * 10 + n
        go(src, dst, az_send.at[i, k], az_recv.at[i, k], outer if n < 4 else inner)

    def wait(i, kb, n):
        k = kb * 10 + n
        arrived(landing(i, kb, n), az_send.at[i, k], az_recv.at[i, k], outer if n < 4 else inner)

    def pass_on(i, kb, got, n):
        wait(i, kb, got)
        src = landing(i, kb, got)
        over(i, kb, n, src, passing(i, kb, 2) if n == 6 else src if got != 5 and got != 6 else
             mine(i, kb, 1 if got == 5 else 2))

    def own(i, kb):
        if kb == 0:
            load(i, 0).wait()
            load(i, 1).wait()
        else:
            arrived(mine(i, 1, 0), ax_send.at[0, i], ax_recv.at[0, i], partner)
            arrived(theirs(i, 1), ax_send.at[1, i], ax_recv.at[1, i], partner)
        over(i, kb, 5, theirs(i, kb), passing(i, kb, 1))
        over(i, kb, 1, mine(i, kb, 0), passing(i, kb, 0))
        over(i, kb, 4, mine(i, kb, 0), mine(i, kb, 0))
        over(i, kb, 0, theirs(i, kb), mine(i, kb, 0))

    def step(i, t):
        for kb in range(2):
            if t == 1:
                pass_on(i, kb, 1, 6)
                pass_on(i, kb, 5, 2)
                pass_on(i, kb, 0, 7)
            elif t == 2:
                pass_on(i, kb, 6, 3)
                pass_on(i, kb, 2, 8)
            elif t == 3:
                pass_on(i, kb, 3, 9)
            elif t == 4:
                wait(i, kb, 4)
                wait(i, kb, 7)
                wait(i, kb, 8)
            else:
                wait(i, kb, 9)

    def first(g, d):
        return at_x(d) if g == 0 else at_y(d)

    def second(g, d):
        return at_y(d) if g == 0 else at_x(d)

    def block(g, d1, d2, who=None):
        dx, dy = (d1, d2) if g == 0 else (d2, d1)
        there = (x + dx + 4) % 4
        who = core if who is None else who
        return b.at[g, (there // 2) * 8 + ((y + dy + 4) % 4) * 2 + who, there % 2]

    load_rot = pltpu.make_async_copy(rot, block(0, 0, 0), load_sem.at[0, N])

    def to_sibling(g, j, k):
        ref = block(g, NEAR[j], NEAR[k])
        go(ref, ref, bs_send.at[g, j * 4 + k], bs_recv.at[g, j * 4 + k], sibling)

    def to_second(g, j):
        ref = block(g, NEAR[j], 0)
        for d in range(2):
            n = j * 4 + d
            go(ref, ref, b2_send.at[g, n], b2_recv.at[g, n], second(g, 1 - 2 * d))
        to_sibling(g, j, 0)

    def b_out():
        load_rot.wait()
        go(block(0, 0, 0), block(1, 0, 0), bz_send, bz_recv, outer)

    def b_start(g):
        ref = block(g, 0, 0)
        if g == 1:
            arrived(ref, bz_send, bz_recv, outer)
        for d in range(2):
            go(ref, ref, b1_send.at[g, d], b1_recv.at[g, d], first(g, 1 - 2 * d))
        to_second(g, 0)

    def b_first(g):
        for d in range(2):
            ref = block(g, 2 * d - 1, 0)
            arrived(ref, b1_send.at[g, d], b1_recv.at[g, d], first(g, 1 - 2 * d))
            part = ref.at[d]
            go(part, part, b1_send.at[g, 2 + d], b1_recv.at[g, 2 + d], first(g, 1 - 2 * d))
            to_second(g, 1 + d)

    def b_far(g):
        for d in range(2):
            arrived(block(g, 2, 0).at[d], b1_send.at[g, 2 + d], b1_recv.at[g, 2 + d],
                    first(g, 1 - 2 * d))
        to_second(g, 3)

    def b_second(g, j):
        for d in range(2):
            n = j * 4 + d
            ref = block(g, NEAR[j], 2 * d - 1)
            arrived(ref, b2_send.at[g, n], b2_recv.at[g, n], second(g, 1 - 2 * d))
            part = ref.at[d]
            go(part, part, b2_send.at[g, n + 2], b2_recv.at[g, n + 2], second(g, 1 - 2 * d))
            to_sibling(g, j, 1 + d)

    def b_last(g, j):
        for d in range(2):
            n = j * 4 + 2 + d
            arrived(block(g, NEAR[j], 2).at[d], b2_send.at[g, n], b2_recv.at[g, n],
                    second(g, 1 - 2 * d))
        to_sibling(g, j, 3)

    def b_sibling(g):
        for j in range(4):
            for k in range(4):
                arrived(block(g, NEAR[j], NEAR[k], 1 - core),
                        bs_send.at[g, j * 4 + k], bs_recv.at[g, j * 4 + k], sibling)

    def compute(i, low, high):
        r = CHUNKS[i]
        if low == 0:
            acc[:, : 2 * r, :] = jnp.zeros((4, 2 * r, 2 * W), jnp.float32)

        def body(m, carry):
            place = plane(((m + 1) // 2) * (2 * (m % 2) - 1))
            lhs = [
                a[side * 8 + place, :, rows(i), :].reshape(2 * r, W) for side in (0, 1)
            ]
            for g in range(2):
                for n in range(2):
                    which = xl if n == 0 else 1 - xl
                    for cd in range(2):
                        total = acc[g * 2 + n, : 2 * r, cd * W : (cd + 1) * W]
                        for side in (0, 1):
                            total = total + jnp.dot(
                                lhs[side], b[g, side * 8 + place, which, cd],
                                preferred_element_type=jnp.float32)
                        acc[g * 2 + n, : 2 * r, cd * W : (cd + 1) * W] = total
            return carry

        lax.fori_loop(low, high, body, 0)

    def out_rows(i, half, quarter):
        return out.at[:, rows(i, half * HALF + quarter * QUARTER), :]

    def store_own(i):
        return pltpu.make_async_copy(
            cs.at[0, :, rows(i), :], out_rows(i, xl, kind), c_local.at[i])

    AWAY = ((3, across), (2, outer), (1, partner))

    def finish(i):
        r = CHUNKS[i]
        for n in (3, 2, 1, 0):
            cs[n, 0, rows(i), :] = (acc[n, :r, :W] - acc[n, r : 2 * r, W:]).astype(jnp.bfloat16)
            cs[n, 1, rows(i), :] = (acc[n, :r, W:] + acc[n, r : 2 * r, :W]).astype(jnp.bfloat16)
        for n, where in AWAY:
            go(cs.at[n, :, rows(i), :], out_rows(i, xl, kind), c_send.at[n, i], c_recv.at[n, i], where)
        store_own(i).start()

    for i in range(N):
        load(i, 0).start()
        load(i, 1).start()
        load(i, 2).start()
        load(i, 3).start()
        if i == 0:
            load_rot.start()

    barrier = pltpu.get_barrier_semaphore()
    for where in (at_x(1), at_x(-1), at_y(1), at_y(-1), inner, outer, across, sibling):
        pl.semaphore_signal(barrier, inc=1, device_id=where, device_id_type=MESH)
    pl.semaphore_wait(barrier, 8)

    own(0, 0)
    swap(0)
    b_out()
    b_start(0)
    own(1, 0)
    swap(1)
    swap(2)
    own(0, 1)
    own(2, 0)
    b_start(1)
    step(0, 1)
    b_second(0, 0)
    own(1, 1)
    b_first(0)
    step(1, 1)
    step(0, 2)
    own(2, 1)
    b_far(0)
    b_first(1)
    step(2, 1)
    b_second(1, 0)
    b_second(0, 1)
    step(1, 2)
    step(0, 3)
    b_second(0, 2)
    b_far(1)
    b_second(1, 1)
    step(2, 2)
    step(1, 3)
    b_second(0, 3)
    b_second(1, 2)
    step(2, 3)
    b_last(0, 0)
    b_last(1, 0)
    b_second(1, 3)
    b_last(0, 1)
    b_last(0, 2)
    b_last(1, 1)
    b_last(1, 2)
    b_last(0, 3)
    b_last(1, 3)
    step(0, 4)
    step(0, 5)
    b_sibling(0)
    b_sibling(1)
    compute(0, 0, 8)
    finish(0)
    step(1, 4)
    step(1, 5)
    compute(1, 0, 8)
    finish(1)
    step(2, 4)
    compute(2, 0, 7)
    step(2, 5)
    compute(2, 7, 8)
    finish(2)

    for copy in sent:
        copy.wait_send()
    for i in range(N):
        store_own(i).wait()
        for n, where in AWAY:
            half = xl if n == 2 else 1 - xl
            quarter = kind if n == 1 else 1 - kind
            arrived(out_rows(i, half, quarter), c_send.at[n, i], c_recv.at[n, i], where)


def local(waves, rotation):
    dma = pltpu.SemaphoreType.DMA
    bf16 = jnp.bfloat16
    return pl.pallas_call(
        kernel,
        out_shape=jax.ShapeDtypeStruct(waves.shape, waves.dtype),
        in_specs=[pl.BlockSpec(memory_space=pl.ANY)] * 2,
        out_specs=pl.BlockSpec(memory_space=pl.ANY),
        scratch_shapes=[
            pltpu.VMEM((16, 2, QUARTER, W), bf16),
            pltpu.VMEM((2, 2, QUARTER, W), bf16),
            pltpu.VMEM((3, 2, 2, QUARTER, W), bf16),
            pltpu.VMEM((2, 2, QUARTER, W), bf16),
            pltpu.VMEM((2, 16, 2, 2, W, W), bf16),
            pltpu.VMEM((4, 2, QUARTER, W), bf16),
            pltpu.VMEM((4, 2 * max(CHUNKS), 2 * W), jnp.float32),
            dma((4, N + 1)),
            dma((2, N)), dma((2, N)),
            dma((N, 20)), dma((N, 20)),
            dma, dma,
            dma((2, 4)), dma((2, 4)),
            dma((2, 16)), dma((2, 16)),
            dma((2, 16)), dma((2, 16)),
            dma((4, N)), dma((4, N)), dma((N,)),
        ],
        compiler_params=pltpu.CompilerParams(
            collective_id=0, has_side_effects=True, vmem_limit_bytes=60 * 1024 * 1024),
        name="rotate",
    )(waves, rotation)


def solution(mesh):
    finer = Mesh(
        mesh.devices.reshape(2, 4, 2, 2, 8), ("xh", "y", "core", "xl", "z")
    )
    return jax.shard_map(
        local,
        mesh=finer,
        in_specs=(P(None, GA, BAND), P(None, GA, BAND)),
        out_specs=P(None, GA, BAND),
        check_vma=False,
    )
```

```python
import jax
import jax.numpy as jnp
from jax import lax
from jax.experimental import pallas as pl
from jax.experimental.pallas import tpu as pltpu
from jax.sharding import Mesh
from jax.sharding import PartitionSpec as P

GA = ("xh", "y", "core")
BAND = ("xl", "z")
MESH = pl.DeviceIdType.MESH

CHUNKS = (96, 96, 64)
PARTS = ((0, 96), (96, 96), (192, 64))
STARTS = tuple(sum(CHUNKS[:i]) for i in range(len(CHUNKS)))
N = len(CHUNKS)
HALF = 512
QUARTER = 256
W = 256
NEAR = (0, -1, 1, 2)


def kernel(
    waves, rot, out,
    a, u, via, xs, b, cs, acc,
    load_sem, ax_send, ax_recv, az_send, az_recv,
    bz_send, bz_recv, b1_send, b1_recv, b2_send, b2_recv, bs_send, bs_recv,
    c_send, c_recv,
):
    xh, y, core = lax.axis_index("xh"), lax.axis_index("y"), lax.axis_index("core")
    xl, z = lax.axis_index("xl"), lax.axis_index("z")
    x = xh * 2 + xl
    s = 1 - 2 * (z % 2)
    kind = (z // 2) % 2

    def plane(d):
        return (z + s * d + 8) % 8

    def at_x(dx):
        there = (x + dx + 4) % 4
        return {"xh": there // 2, "xl": there % 2}

    def at_y(dy):
        return {"y": (y + dy + 4) % 4}

    inner = {"z": plane(1)}
    outer = {"z": plane(-1)}
    partner = {"xl": 1 - xl}
    across = {"xl": 1 - xl, "z": plane(-1)}
    sibling = {"core": 1 - core}

    def rows(i, base=0):
        return pl.ds(base + STARTS[i], CHUNKS[i])

    def remote(src, dst, send, recv, where):
        return pltpu.make_async_remote_copy(
            src_ref=src, dst_ref=dst, send_sem=send, recv_sem=recv,
            device_id=where, device_id_type=MESH,
        )

    sent = []

    def go(src, dst, send, recv, where):
        copy = remote(src, dst, send, recv, where)
        copy.start()
        sent.append(copy)

    def arrived(dst, send, recv, where):
        remote(dst, dst, send, recv, where).wait_recv()

    def mine(i, kb, d):
        side = xl if kb == 0 else 1 - xl
        return a.at[side * 8 + plane(d), :, rows(i), :]

    def theirs(i, kb):
        return u.at[kb, :, rows(i), :]

    def passing(i, kb, j):
        return via.at[j, kb, :, rows(i), :]

    def spare(i, j):
        return xs.at[j, :, rows(i), :]

    def load(i, j):
        half = xl if j < 2 else 1 - xl
        quarter = kind if j % 2 == 0 else 1 - kind
        dst = (mine(i, 0, 0), theirs(i, 0), spare(i, 0), spare(i, 1))[j]
        return pltpu.make_async_copy(
            waves.at[:, rows(i, half * HALF + quarter * QUARTER), :], dst, load_sem.at[j, i])

    def swap(i):
        load(i, 2).wait()
        go(spare(i, 0), mine(i, 0, 0), ax_send.at[0, i], ax_recv.at[0, i], partner)
        load(i, 3).wait()
        go(spare(i, 1), theirs(i, 1), ax_send.at[1, i], ax_recv.at[1, i], partner)

    def landing(i, kb, n):
        if n == 1:
            return passing(i, kb, 0)
        if n == 5:
            return passing(i, kb, 1)
        if n == 6:
            return passing(i, kb, 2)
        return mine(i, kb, {0: -1, 2: -2, 3: -3, 4: 1, 7: 2, 8: 3, 9: 4}[n])

    def over(i, kb, n, src, dst):
        k = kb * 10 + n
        go(src, dst, az_send.at[i, k], az_recv.at[i, k], outer if n < 4 else inner)

    def wait(i, kb, n):
        k = kb * 10 + n
        arrived(landing(i, kb, n), az_send.at[i, k], az_recv.at[i, k], outer if n < 4 else inner)

    def pass_on(i, kb, got, n):
        wait(i, kb, got)
        src = landing(i, kb, got)
        over(i, kb, n, src, passing(i, kb, 2) if n == 6 else src if got != 5 and got != 6 else
             mine(i, kb, 1 if got == 5 else 2))

    def own(i, kb):
        if kb == 0:
            load(i, 0).wait()
            load(i, 1).wait()
        else:
            arrived(mine(i, 1, 0), ax_send.at[0, i], ax_recv.at[0, i], partner)
            arrived(theirs(i, 1), ax_send.at[1, i], ax_recv.at[1, i], partner)
        over(i, kb, 5, theirs(i, kb), passing(i, kb, 1))
        over(i, kb, 1, mine(i, kb, 0), passing(i, kb, 0))
        over(i, kb, 4, mine(i, kb, 0), mine(i, kb, 0))
        over(i, kb, 0, theirs(i, kb), mine(i, kb, 0))

    def first(g, d):
        return at_x(d) if g == 0 else at_y(d)

    def second(g, d):
        return at_y(d) if g == 0 else at_x(d)

    def block(g, d1, d2, who=None):
        dx, dy = (d1, d2) if g == 0 else (d2, d1)
        there = (x + dx + 4) % 4
        who = core if who is None else who
        return b.at[g, (there // 2) * 8 + ((y + dy + 4) % 4) * 2 + who, there % 2]

    load_rot = pltpu.make_async_copy(rot, block(0, 0, 0), load_sem.at[0, N])

    def to_sibling(g, j, k):
        ref = block(g, NEAR[j], NEAR[k])
        go(ref, ref, bs_send.at[g, j * 4 + k], bs_recv.at[g, j * 4 + k], sibling)

    def to_second(g, j):
        ref = block(g, NEAR[j], 0)
        for d in range(2):
            n = j * 4 + d
            go(ref, ref, b2_send.at[g, n], b2_recv.at[g, n], second(g, 1 - 2 * d))
        to_sibling(g, j, 0)

    def b_out():
        load_rot.wait()
        go(block(0, 0, 0), block(1, 0, 0), bz_send, bz_recv, outer)

    def b_start(g):
        ref = block(g, 0, 0)
        if g == 1:
            arrived(ref, bz_send, bz_recv, outer)
        for d in range(2):
            go(ref, ref, b1_send.at[g, d], b1_recv.at[g, d], first(g, 1 - 2 * d))
        to_second(g, 0)

    def b_first(g, d):
        ref = block(g, 2 * d - 1, 0)
        arrived(ref, b1_send.at[g, d], b1_recv.at[g, d], first(g, 1 - 2 * d))
        part = ref.at[d]
        go(part, part, b1_send.at[g, 2 + d], b1_recv.at[g, 2 + d], first(g, 1 - 2 * d))
        to_second(g, 1 + d)

    def b_far(g):
        for d in range(2):
            arrived(block(g, 2, 0).at[d], b1_send.at[g, 2 + d], b1_recv.at[g, 2 + d],
                    first(g, 1 - 2 * d))
        to_second(g, 3)

    def b_second(g, j, d):
        n = j * 4 + d
        ref = block(g, NEAR[j], 2 * d - 1)
        arrived(ref, b2_send.at[g, n], b2_recv.at[g, n], second(g, 1 - 2 * d))
        part = ref.at[d]
        go(part, part, b2_send.at[g, n + 2], b2_recv.at[g, n + 2], second(g, 1 - 2 * d))
        to_sibling(g, j, 1 + d)

    def b_last(g, j):
        for d in range(2):
            n = j * 4 + 2 + d
            arrived(block(g, NEAR[j], 2).at[d], b2_send.at[g, n], b2_recv.at[g, n],
                    second(g, 1 - 2 * d))
        to_sibling(g, j, 3)

    def b_sibling(g):
        for j in range(4):
            for k in range(4):
                arrived(block(g, NEAR[j], NEAR[k], 1 - core),
                        bs_send.at[g, j * 4 + k], bs_recv.at[g, j * 4 + k], sibling)

    def compute(p, g, low, high):
        base, r = PARTS[p]
        here = pl.ds(base, r)
        if low == 0:
            acc[2 * g : 2 * g + 2, pl.ds(2 * base, 2 * r), :] = jnp.zeros((2, 2 * r, 2 * W), jnp.float32)

        def body(m, carry):
            place = plane(((m + 1) // 2) * (2 * (m % 2) - 1))
            lhs = [a[side * 8 + place, :, here, :].reshape(2 * r, W) for side in (0, 1)]
            for n in range(2):
                which = xl if n == 0 else 1 - xl
                for cd in range(2):
                    total = acc[g * 2 + n, pl.ds(2 * base, 2 * r), cd * W : (cd + 1) * W]
                    for side in (0, 1):
                        total = total + jnp.dot(
                            lhs[side], b[g, side * 8 + place, which, cd],
                            preferred_element_type=jnp.float32)
                    acc[g * 2 + n, pl.ds(2 * base, 2 * r), cd * W : (cd + 1) * W] = total
            return carry

        lax.fori_loop(low, high, body, 0, unroll=high - low)

    def out_rows(p, half, quarter):
        base, r = PARTS[p]
        return out.at[:, pl.ds(base + half * HALF + quarter * QUARTER, r), :]

    def result(n, p):
        base, r = PARTS[p]
        return cs.at[n, :, pl.ds(base, r), :]

    AWAY = ((3, across), (2, outer), (1, partner))

    def finish(p, g):
        base, r = PARTS[p]
        here = pl.ds(base, r)
        for n in (2 * g + 1, 2 * g):
            top, low = pl.ds(2 * base, r), pl.ds(2 * base + r, r)
            dst = out_rows(p, xl, kind) if n == 0 else result(n, p)
            dst[0] = (acc[n, top, :W] - acc[n, low, W:]).astype(jnp.bfloat16)
            dst[1] = (acc[n, top, W:] + acc[n, low, :W]).astype(jnp.bfloat16)
        for n, where in AWAY:
            if n // 2 == g:
                go(result(n, p), out_rows(p, xl, kind), c_send.at[n, p], c_recv.at[n, p], where)

    for i in range(N):
        load(i, 0).start()
        load(i, 1).start()
        load(i, 2).start()
        load(i, 3).start()
        if i == 0:
            load_rot.start()

    barrier = pltpu.get_barrier_semaphore()
    for where in (at_x(1), at_x(-1), at_y(1), at_y(-1), inner, outer, across, sibling):
        pl.semaphore_signal(barrier, inc=1, device_id=where, device_id_type=MESH)
    pl.semaphore_wait(barrier, 8)

    b_out()
    b_start(0)
    swap(0)
    own(0, 0)
    swap(1)
    swap(2)
    own(1, 0)
    pass_on(0, 0, 5, 2)
    own(2, 0)
    b_start(1)
    b_second(0, 0, 0)
    b_second(0, 0, 1)
    b_first(0, 0)
    b_first(0, 1)
    pass_on(1, 0, 5, 2)
    pass_on(0, 0, 1, 6)
    pass_on(0, 0, 0, 7)
    pass_on(2, 0, 5, 2)
    own(0, 1)
    pass_on(1, 0, 1, 6)
    b_first(1, 0)
    b_first(1, 1)
    pass_on(0, 0, 6, 3)
    pass_on(1, 0, 0, 7)
    pass_on(0, 0, 2, 8)
    b_last(0, 0)
    pass_on(2, 0, 1, 6)
    pass_on(0, 1, 5, 2)
    pass_on(2, 0, 0, 7)
    pass_on(1, 0, 2, 8)
    b_second(0, 1, 0)
    b_second(0, 1, 1)
    pass_on(1, 0, 6, 3)
    pass_on(2, 0, 2, 8)
    b_second(1, 0, 0)
    b_second(1, 0, 1)
    pass_on(0, 1, 1, 6)
    b_far(0)
    pass_on(0, 1, 0, 7)
    b_second(0, 2, 0)
    b_second(0, 2, 1)
    pass_on(2, 0, 6, 3)
    pass_on(0, 0, 3, 9)
    b_far(1)
    pass_on(0, 1, 2, 8)
    b_second(1, 1, 0)
    b_second(1, 1, 1)
    pass_on(1, 0, 3, 9)
    b_last(0, 1)
    pass_on(2, 0, 3, 9)
    pass_on(0, 1, 6, 3)
    b_second(1, 2, 0)
    b_second(1, 2, 1)
    b_second(0, 3, 0)
    b_second(0, 3, 1)
    pass_on(0, 1, 3, 9)
    b_last(1, 0)
    b_last(0, 2)
    own(1, 1)
    b_last(0, 3)
    b_second(1, 3, 0)
    b_second(1, 3, 1)
    b_sibling(0)
    wait(0, 0, 4)
    wait(0, 1, 4)
    wait(0, 0, 7)
    wait(0, 1, 7)
    compute(0, 0, 0, 4)
    pass_on(1, 1, 1, 6)
    wait(0, 0, 8)
    wait(0, 1, 8)
    compute(0, 0, 4, 7)
    wait(0, 0, 9)
    wait(0, 1, 9)
    compute(0, 0, 7, 8)
    finish(0, 0)
    b_last(1, 1)
    pass_on(1, 1, 5, 2)
    own(2, 1)
    pass_on(1, 1, 0, 7)
    b_last(1, 2)
    pass_on(1, 1, 6, 3)
    pass_on(1, 1, 2, 8)
    b_last(1, 3)
    pass_on(2, 1, 5, 2)
    pass_on(2, 1, 1, 6)
    b_sibling(1)
    compute(0, 1, 0, 4)
    pass_on(2, 1, 0, 7)
    compute(0, 1, 4, 7)
    compute(0, 1, 7, 8)
    finish(0, 1)
    wait(1, 0, 4)
    wait(1, 1, 4)
    wait(1, 0, 7)
    wait(1, 1, 7)
    compute(1, 1, 0, 4)
    pass_on(1, 1, 3, 9)
    compute(1, 0, 0, 4)
    pass_on(2, 1, 2, 8)
    wait(1, 0, 8)
    wait(1, 1, 8)
    compute(1, 1, 4, 7)
    compute(1, 0, 4, 7)
    pass_on(2, 1, 6, 3)
    wait(2, 0, 4)
    wait(2, 1, 4)
    wait(2, 0, 7)
    wait(2, 1, 7)
    compute(2, 1, 0, 4)
    compute(2, 0, 0, 4)
    wait(1, 0, 9)
    wait(1, 1, 9)
    compute(1, 1, 7, 8)
    finish(1, 1)
    pass_on(2, 1, 3, 9)
    compute(1, 0, 7, 8)
    finish(1, 0)
    wait(2, 0, 8)
    wait(2, 1, 8)
    compute(2, 1, 4, 7)
    compute(2, 0, 4, 7)
    wait(2, 0, 9)
    wait(2, 1, 9)
    compute(2, 1, 7, 8)
    finish(2, 1)
    compute(2, 0, 7, 8)
    finish(2, 0)

    for copy in sent:
        copy.wait_send()
    for p in range(len(PARTS)):
        for n, where in AWAY:
            half = xl if n == 2 else 1 - xl
            quarter = kind if n == 1 else 1 - kind
            arrived(out_rows(p, half, quarter), c_send.at[n, p], c_recv.at[n, p], where)


def local(waves, rotation):
    dma = pltpu.SemaphoreType.DMA
    bf16 = jnp.bfloat16
    return pl.pallas_call(
        kernel,
        out_shape=pltpu.VMEM(waves.shape, waves.dtype),
        in_specs=[pl.BlockSpec(memory_space=pl.ANY)] * 2,
        out_specs=pl.BlockSpec(memory_space=pltpu.VMEM),
        scratch_shapes=[
            pltpu.VMEM((16, 2, QUARTER, W), bf16),
            pltpu.VMEM((2, 2, QUARTER, W), bf16),
            pltpu.VMEM((3, 2, 2, QUARTER, W), bf16),
            pltpu.VMEM((2, 2, QUARTER, W), bf16),
            pltpu.VMEM((2, 16, 2, 2, W, W), bf16),
            pltpu.VMEM((4, 2, QUARTER, W), bf16),
            pltpu.VMEM((4, 2 * QUARTER, 2 * W), jnp.float32),
            dma((4, N + 1)),
            dma((2, N)), dma((2, N)),
            dma((N, 20)), dma((N, 20)),
            dma, dma,
            dma((2, 4)), dma((2, 4)),
            dma((2, 16)), dma((2, 16)),
            dma((2, 16)), dma((2, 16)),
            dma((4, N)), dma((4, N)),
        ],
        compiler_params=pltpu.CompilerParams(
            collective_id=0, has_side_effects=True, vmem_limit_bytes=60 * 1024 * 1024),
        name="rotate",
    )(waves, rotation)


def solution(mesh):
    finer = Mesh(
        mesh.devices.reshape(2, 4, 2, 2, 8), ("xh", "y", "core", "xl", "z")
    )
    return jax.shard_map(
        local,
        mesh=finer,
        in_specs=(P(None, GA, BAND), P(None, GA, BAND)),
        out_specs=P(None, GA, BAND),
        check_vma=False,
    )
```

```python
import jax
import jax.numpy as jnp
from jax import lax
from jax.experimental import pallas as pl
from jax.experimental.pallas import tpu as pltpu
from jax.sharding import Mesh
from jax.sharding import PartitionSpec as P

GA = ("xh", "y", "core")
BAND = ("xl", "z")
MESH = pl.DeviceIdType.MESH

CHUNKS = (96, 96, 64)
PARTS = ((0, 96), (96, 96), (192, 64))
STARTS = tuple(sum(CHUNKS[:i]) for i in range(len(CHUNKS)))
N = len(CHUNKS)
HALF = 512
QUARTER = 256
W = 256
NEAR = (0, -1, 1, 2)


def kernel(
    waves, rot, out,
    a, u, via, xs, b, cs, acc,
    load_sem, send_sem, ax_sem, az_sem, bz_sem, b1_sem, b2_sem, bs_sem, c_sem,
):
    xh, y, core = lax.axis_index("xh"), lax.axis_index("y"), lax.axis_index("core")
    xl, z = lax.axis_index("xl"), lax.axis_index("z")
    x = xh * 2 + xl
    s = 1 - 2 * (z % 2)
    kind = (z // 2) % 2

    def plane(d):
        return (z + s * d + 8) % 8

    def at_x(dx):
        there = (x + dx + 4) % 4
        return {"xh": there // 2, "xl": there % 2}

    def at_y(dy):
        return {"y": (y + dy + 4) % 4}

    inner = {"z": plane(1)}
    outer = {"z": plane(-1)}
    partner = {"xl": 1 - xl}
    across = {"xl": 1 - xl, "z": plane(-1)}
    sibling = {"core": 1 - core}

    def rows(i, base=0):
        return pl.ds(base + STARTS[i], CHUNKS[i])

    def remote(src, dst, send, recv, where):
        return pltpu.make_async_remote_copy(
            src_ref=src, dst_ref=dst, send_sem=send, recv_sem=recv,
            device_id=where, device_id_type=MESH,
        )

    def go(src, dst, recv, where, group=0):
        remote(src, dst, send_sem.at[group], recv, where).start()

    def arrived(ref, recv):
        remote(ref, ref, send_sem.at[0], recv, sibling).wait_recv()

    def mine(i, kb, d):
        side = xl if kb == 0 else 1 - xl
        return a.at[side * 8 + plane(d), :, rows(i), :]

    def theirs(i, kb):
        return u.at[kb, :, rows(i), :]

    def passing(i, kb, j):
        return via.at[j, kb, :, rows(i), :]

    def spare(i, j):
        return xs.at[j, :, rows(i), :]

    def load(i, j):
        half = xl if j < 2 else 1 - xl
        quarter = kind if j % 2 == 0 else 1 - kind
        dst = (mine(i, 0, 0), theirs(i, 0), spare(i, 0), spare(i, 1))[j]
        return pltpu.make_async_copy(
            waves.at[:, rows(i, half * HALF + quarter * QUARTER), :], dst, load_sem.at[j // 2, i])

    def both(ref, i):
        return ref.at[:, :, rows(i), :]

    def loaded(i, j):
        pltpu.make_async_copy(both(u, i), both(u, i), load_sem.at[j, i]).wait()

    def swap(i):
        loaded(i, 1)
        go(spare(i, 0), mine(i, 0, 0), ax_sem.at[i], partner)
        go(spare(i, 1), theirs(i, 1), ax_sem.at[i], partner)

    def landing(i, kb, n):
        if n == 1:
            return passing(i, kb, 0)
        if n == 5:
            return passing(i, kb, 1)
        if n == 6:
            return passing(i, kb, 2)
        return mine(i, kb, {0: -1, 2: -2, 3: -3, 4: 1, 7: 2, 8: 3, 9: 4}[n])

    def mark(i, kb, n):
        last = {4: 12, 7: 12, 8: 13, 9: 14}
        return az_sem.at[i, last[n] if n in last else kb * 6 + (0, 1, 2, 3, 5, 6).index(n)]

    def over(i, kb, n, src, dst):
        go(src, dst, mark(i, kb, n), outer if n < 4 else inner)

    def wait(i, kb, n):
        arrived(landing(i, kb, n), mark(i, kb, n))

    def settle(i, n):
        arrived(via.at[0:2, :, :, rows(i), :] if n == 4 else both(u, i), mark(i, 0, n))

    def pass_on(i, kb, got, n):
        wait(i, kb, got)
        src = landing(i, kb, got)
        over(i, kb, n, src, passing(i, kb, 2) if n == 6 else src if got != 5 and got != 6 else
             mine(i, kb, 1 if got == 5 else 2))

    def own(i, kb):
        if kb == 0:
            loaded(i, 0)
        else:
            arrived(both(u, i), ax_sem.at[i])
        over(i, kb, 5, theirs(i, kb), passing(i, kb, 1))
        over(i, kb, 1, mine(i, kb, 0), passing(i, kb, 0))
        over(i, kb, 4, mine(i, kb, 0), mine(i, kb, 0))
        over(i, kb, 0, theirs(i, kb), mine(i, kb, 0))

    def first(g, d):
        return at_x(d) if g == 0 else at_y(d)

    def second(g, d):
        return at_y(d) if g == 0 else at_x(d)

    def block(g, d1, d2, who=None):
        dx, dy = (d1, d2) if g == 0 else (d2, d1)
        there = (x + dx + 4) % 4
        who = core if who is None else who
        return b.at[(g * 16 + (there // 2) * 8 + ((y + dy + 4) % 4) * 2 + who) * 2 + there % 2]

    load_rot = pltpu.make_async_copy(rot, block(0, 0, 0), load_sem.at[0, N])

    def to_sibling(g, j, k):
        ref = block(g, NEAR[j], NEAR[k])
        go(ref, ref, bs_sem.at[g], sibling, 1)

    def to_second(g, j):
        ref = block(g, NEAR[j], 0)
        for d in range(2):
            go(ref, ref, b2_sem.at[g, j, d], second(g, 1 - 2 * d), 1)
        to_sibling(g, j, 0)

    def b_out():
        load_rot.wait()
        go(block(0, 0, 0), block(1, 0, 0), bz_sem, outer)

    def b_start(g):
        ref = block(g, 0, 0)
        if g == 1:
            arrived(ref, bz_sem)
        for d in range(2):
            go(ref, ref, b1_sem.at[g, d], first(g, 1 - 2 * d))
        to_second(g, 0)

    def b_first(g, d):
        ref = block(g, 2 * d - 1, 0)
        arrived(ref, b1_sem.at[g, d])
        go(ref.at[d], ref.at[d], b1_sem.at[g, 2], first(g, 1 - 2 * d))
        to_second(g, 1 + d)

    def b_far(g):
        arrived(block(g, 2, 0), b1_sem.at[g, 2])
        to_second(g, 3)

    def b_second(g, j, d):
        ref = block(g, NEAR[j], 2 * d - 1)
        arrived(ref, b2_sem.at[g, j, d])
        go(ref.at[d], ref.at[d], b2_sem.at[g, j, 2], second(g, 1 - 2 * d), 1)
        to_sibling(g, j, 1 + d)

    def b_last(g, j):
        arrived(block(g, NEAR[j], 2), b2_sem.at[g, j, 2])
        to_sibling(g, j, 3)

    def b_sibling(g):
        arrived(b.at[0:16], bs_sem.at[g])

    def compute(p, g, low, high):
        base, r = PARTS[p]
        here = pl.ds(base, r)
        if low == 0:
            acc[2 * g : 2 * g + 2, pl.ds(2 * base, 2 * r), :] = jnp.zeros((2, 2 * r, 2 * W), jnp.float32)

        def body(m, carry):
            place = plane(((m + 1) // 2) * (2 * (m % 2) - 1))
            lhs = [a[side * 8 + place, :, here, :].reshape(2 * r, W) for side in (0, 1)]
            for n in range(2):
                which = xl if n == 0 else 1 - xl
                for cd in range(2):
                    total = acc[g * 2 + n, pl.ds(2 * base, 2 * r), cd * W : (cd + 1) * W]
                    for side in (0, 1):
                        total = total + jnp.dot(
                            lhs[side], b[(g * 16 + side * 8 + place) * 2 + which, cd],
                            preferred_element_type=jnp.float32)
                    acc[g * 2 + n, pl.ds(2 * base, 2 * r), cd * W : (cd + 1) * W] = total
            return carry

        lax.fori_loop(low, high, body, 0, unroll=high - low)

    def out_rows(p, half, quarter):
        base, r = PARTS[p]
        return out.at[:, pl.ds(base + half * HALF + quarter * QUARTER, r), :]

    def result(n, p):
        base, r = PARTS[p]
        return cs.at[n, :, pl.ds(base, r), :]

    AWAY = ((3, across), (2, outer), (1, partner))

    def finish(p, g):
        base, r = PARTS[p]
        here = pl.ds(base, r)
        for n in (2 * g + 1, 2 * g):
            top, low = pl.ds(2 * base, r), pl.ds(2 * base + r, r)
            dst = out_rows(p, xl, kind) if n == 0 else result(n, p)
            dst[0] = (acc[n, top, :W] - acc[n, low, W:]).astype(jnp.bfloat16)
            dst[1] = (acc[n, top, W:] + acc[n, low, :W]).astype(jnp.bfloat16)
        for n, where in AWAY:
            if n // 2 == g:
                go(result(n, p), out_rows(p, xl, kind), c_sem, where)

    for i in range(N):
        load(i, 0).start()
        load(i, 1).start()
        load(i, 2).start()
        load(i, 3).start()
        if i == 0:
            load_rot.start()

    barrier = pltpu.get_barrier_semaphore()
    for where in (at_x(1), at_x(-1), at_y(1), at_y(-1), inner, outer, across, sibling):
        pl.semaphore_signal(barrier, inc=1, device_id=where, device_id_type=MESH)
    pl.semaphore_wait(barrier, 8)

    b_out()
    b_start(0)
    swap(0)
    own(0, 0)
    swap(1)
    swap(2)
    own(1, 0)
    pass_on(0, 0, 5, 2)
    own(2, 0)
    b_start(1)
    b_second(0, 0, 0)
    b_second(0, 0, 1)
    b_first(0, 0)
    b_first(0, 1)
    pass_on(1, 0, 5, 2)
    pass_on(0, 0, 1, 6)
    pass_on(0, 0, 0, 7)
    pass_on(2, 0, 5, 2)
    own(0, 1)
    pass_on(1, 0, 1, 6)
    b_first(1, 0)
    b_first(1, 1)
    pass_on(0, 0, 6, 3)
    pass_on(1, 0, 0, 7)
    pass_on(0, 0, 2, 8)
    b_last(0, 0)
    pass_on(2, 0, 1, 6)
    pass_on(0, 1, 5, 2)
    pass_on(2, 0, 0, 7)
    pass_on(1, 0, 2, 8)
    b_second(0, 1, 0)
    b_second(0, 1, 1)
    pass_on(1, 0, 6, 3)
    pass_on(2, 0, 2, 8)
    b_second(1, 0, 0)
    b_second(1, 0, 1)
    pass_on(0, 1, 1, 6)
    b_far(0)
    pass_on(0, 1, 0, 7)
    b_second(0, 2, 0)
    b_second(0, 2, 1)
    pass_on(2, 0, 6, 3)
    pass_on(0, 0, 3, 9)
    b_far(1)
    pass_on(0, 1, 2, 8)
    b_second(1, 1, 0)
    b_second(1, 1, 1)
    pass_on(1, 0, 3, 9)
    b_last(0, 1)
    pass_on(2, 0, 3, 9)
    pass_on(0, 1, 6, 3)
    b_second(1, 2, 0)
    b_second(1, 2, 1)
    b_second(0, 3, 0)
    b_second(0, 3, 1)
    pass_on(0, 1, 3, 9)
    b_last(1, 0)
    b_last(0, 2)
    own(1, 1)
    b_last(0, 3)
    b_second(1, 3, 0)
    b_second(1, 3, 1)
    b_sibling(0)
    settle(0, 4)
    compute(0, 0, 0, 4)
    pass_on(1, 1, 1, 6)
    settle(0, 8)
    compute(0, 0, 4, 7)
    settle(0, 9)
    compute(0, 0, 7, 8)
    finish(0, 0)
    b_last(1, 1)
    pass_on(1, 1, 5, 2)
    own(2, 1)
    pass_on(1, 1, 0, 7)
    b_last(1, 2)
    pass_on(1, 1, 6, 3)
    pass_on(1, 1, 2, 8)
    b_last(1, 3)
    pass_on(2, 1, 5, 2)
    pass_on(2, 1, 1, 6)
    b_sibling(1)
    compute(0, 1, 0, 4)
    pass_on(2, 1, 0, 7)
    compute(0, 1, 4, 7)
    compute(0, 1, 7, 8)
    finish(0, 1)
    settle(1, 4)
    compute(1, 1, 0, 4)
    pass_on(1, 1, 3, 9)
    compute(1, 0, 0, 4)
    pass_on(2, 1, 2, 8)
    settle(1, 8)
    compute(1, 1, 4, 7)
    compute(1, 0, 4, 7)
    pass_on(2, 1, 6, 3)
    settle(2, 4)
    compute(2, 1, 0, 4)
    compute(2, 0, 0, 4)
    settle(1, 9)
    compute(1, 1, 7, 8)
    finish(1, 1)
    pass_on(2, 1, 3, 9)
    compute(1, 0, 7, 8)
    finish(1, 0)
    settle(2, 8)
    compute(2, 1, 4, 7)
    compute(2, 0, 4, 7)
    settle(2, 9)
    compute(2, 1, 7, 8)
    finish(2, 1)
    compute(2, 0, 7, 8)
    finish(2, 0)

    remote(b.at[0:32], b.at[0:32], send_sem.at[0], c_sem, sibling).wait_send()
    remote(b.at[0:56], b.at[0:56], send_sem.at[1], c_sem, sibling).wait_send()
    arrived(cs.at[0:3], c_sem)


def local(waves, rotation):
    dma = pltpu.SemaphoreType.DMA
    bf16 = jnp.bfloat16
    return pl.pallas_call(
        kernel,
        out_shape=pltpu.VMEM(waves.shape, waves.dtype),
        in_specs=[pl.BlockSpec(memory_space=pl.ANY)] * 2,
        out_specs=pl.BlockSpec(memory_space=pltpu.VMEM),
        scratch_shapes=[
            pltpu.VMEM((16, 2, QUARTER, W), bf16),
            pltpu.VMEM((2, 2, QUARTER, W), bf16),
            pltpu.VMEM((3, 2, 2, QUARTER, W), bf16),
            pltpu.VMEM((2, 2, QUARTER, W), bf16),
            pltpu.VMEM((64, 2, W, W), bf16),
            pltpu.VMEM((4, 2, QUARTER, W), bf16),
            pltpu.VMEM((4, 2 * QUARTER, 2 * W), jnp.float32),
            dma((2, N + 1)), dma((2,)), dma((N,)), dma((N, 15)), dma,
            dma((2, 3)), dma((2, 4, 3)), dma((2,)), dma,
        ],
        compiler_params=pltpu.CompilerParams(
            collective_id=0, has_side_effects=True, vmem_limit_bytes=60 * 1024 * 1024),
        name="rotate",
    )(waves, rotation)


def solution(mesh):
    finer = Mesh(
        mesh.devices.reshape(2, 4, 2, 2, 8), ("xh", "y", "core", "xl", "z")
    )
    return jax.shard_map(
        local,
        mesh=finer,
        in_specs=(P(None, GA, BAND), P(None, GA, BAND)),
        out_specs=P(None, GA, BAND),
        check_vma=False,
    )
```

```python
import jax
import jax.numpy as jnp
from jax import lax
from jax.experimental import pallas as pl
from jax.experimental.pallas import tpu as pltpu
from jax.sharding import Mesh
from jax.sharding import PartitionSpec as P

GA = ("xh", "y", "core")
BAND = ("xl", "z")
MESH = pl.DeviceIdType.MESH

CHUNKS = (96, 96, 64)
PARTS = ((0, 96), (96, 96), (192, 64))
STARTS = tuple(sum(CHUNKS[:i]) for i in range(len(CHUNKS)))
N = len(CHUNKS)
HALF = 512
QUARTER = 256
W = 256
NEAR = (0, -1, 1, 2)


def kernel(
    waves, rot, out,
    a, u, via, xs, b, cs, acc,
    load_sem, send_sem, ax_sem, az_sem, bz_sem, b1_sem, b2_sem, bs_sem, c_sem,
):
    xh, y, core = lax.axis_index("xh"), lax.axis_index("y"), lax.axis_index("core")
    xl, z = lax.axis_index("xl"), lax.axis_index("z")
    x = xh * 2 + xl
    s = 1 - 2 * (z % 2)
    kind = (z // 2) % 2

    def plane(d):
        return (z + s * d + 8) % 8

    def at_x(dx):
        there = (x + dx + 4) % 4
        return {"xh": there // 2, "xl": there % 2}

    def at_y(dy):
        return {"y": (y + dy + 4) % 4}

    inner = {"z": plane(1)}
    outer = {"z": plane(-1)}
    partner = {"xl": 1 - xl}
    across = {"xl": 1 - xl, "z": plane(-1)}
    sibling = {"core": 1 - core}

    def rows(i, base=0):
        return pl.ds(base + STARTS[i], CHUNKS[i])

    def remote(src, dst, send, recv, where):
        return pltpu.make_async_remote_copy(
            src_ref=src, dst_ref=dst, send_sem=send, recv_sem=recv,
            device_id=where, device_id_type=MESH,
        )

    def go(src, dst, recv, where, group=0):
        remote(src, dst, send_sem.at[group], recv, where).start()

    def arrived(ref, recv):
        remote(ref, ref, send_sem.at[0], recv, sibling).wait_recv()

    def mine(i, kb, d):
        side = xl if kb == 0 else 1 - xl
        return a.at[side * 8 + plane(d), :, rows(i), :]

    def theirs(i, kb):
        return u.at[kb, :, rows(i), :]

    def passing(i, kb, j):
        return via.at[j, kb, :, rows(i), :]

    def spare(i, j):
        return xs.at[j, :, rows(i), :]

    def load(i, j):
        half = xl if j < 2 else 1 - xl
        quarter = kind if j % 2 == 0 else 1 - kind
        dst = (mine(i, 0, 0), theirs(i, 0), spare(i, 0), spare(i, 1))[j]
        return pltpu.make_async_copy(
            waves.at[:, rows(i, half * HALF + quarter * QUARTER), :], dst, load_sem.at[j // 2, i])

    def both(ref, i):
        return ref.at[:, :, rows(i), :]

    def loaded(i, j):
        pltpu.make_async_copy(both(u, i), both(u, i), load_sem.at[j, i]).wait()

    def swap(i):
        loaded(i, 1)
        go(spare(i, 0), mine(i, 0, 0), ax_sem.at[i], partner)
        go(spare(i, 1), theirs(i, 1), ax_sem.at[i], partner)

    def landing(i, kb, n):
        if n == 1:
            return passing(i, kb, 0)
        if n == 5:
            return passing(i, kb, 1)
        if n == 6:
            return passing(i, kb, 2)
        return mine(i, kb, {0: -1, 2: -2, 3: -3, 4: 1, 7: 2, 8: 3, 9: 4}[n])

    def mark(i, kb, n):
        last = {4: 12, 7: 12, 8: 13, 9: 14}
        return az_sem.at[i, last[n] if n in last else kb * 6 + (0, 1, 2, 3, 5, 6).index(n)]

    def over(i, kb, n, src, dst):
        go(src, dst, mark(i, kb, n), outer if n < 4 else inner)

    def wait(i, kb, n):
        arrived(landing(i, kb, n), mark(i, kb, n))

    def settle(i, n):
        arrived(via.at[0:2, :, :, rows(i), :] if n == 4 else both(u, i), mark(i, 0, n))

    def pass_on(i, kb, got, n):
        wait(i, kb, got)
        src = landing(i, kb, got)
        over(i, kb, n, src, passing(i, kb, 2) if n == 6 else src if got != 5 and got != 6 else
             mine(i, kb, 1 if got == 5 else 2))

    def own(i, kb):
        if kb == 0:
            loaded(i, 0)
        else:
            arrived(both(u, i), ax_sem.at[i])
        over(i, kb, 5, theirs(i, kb), passing(i, kb, 1))
        over(i, kb, 1, mine(i, kb, 0), passing(i, kb, 0))
        over(i, kb, 4, mine(i, kb, 0), mine(i, kb, 0))
        over(i, kb, 0, theirs(i, kb), mine(i, kb, 0))

    def first(g, d):
        return at_x(d) if g == 0 else at_y(d)

    def second(g, d):
        return at_y(d) if g == 0 else at_x(d)

    def block(g, d1, d2, who=None):
        dx, dy = (d1, d2) if g == 0 else (d2, d1)
        there = (x + dx + 4) % 4
        who = core if who is None else who
        return b.at[(g * 16 + (there // 2) * 8 + ((y + dy + 4) % 4) * 2 + who) * 2 + there % 2]

    load_rot = pltpu.make_async_copy(rot, block(0, 0, 0), load_sem.at[0, N])

    def to_sibling(g, j, k):
        ref = block(g, NEAR[j], NEAR[k])
        go(ref, ref, bs_sem.at[g], sibling, 1)

    def to_second(g, j):
        ref = block(g, NEAR[j], 0)
        for d in range(2):
            go(ref, ref, b2_sem.at[g, j, d], second(g, 1 - 2 * d), 1)
        to_sibling(g, j, 0)

    def b_out():
        load_rot.wait()
        go(block(0, 0, 0), block(1, 0, 0), bz_sem, outer)

    def b_start(g):
        ref = block(g, 0, 0)
        if g == 1:
            arrived(ref, bz_sem)
        for d in range(2):
            go(ref, ref, b1_sem.at[g, d], first(g, 1 - 2 * d))
        to_second(g, 0)

    def b_first(g, d):
        ref = block(g, 2 * d - 1, 0)
        arrived(ref, b1_sem.at[g, d])
        go(ref.at[d], ref.at[d], b1_sem.at[g, 2], first(g, 1 - 2 * d))
        to_second(g, 1 + d)

    def b_far(g):
        arrived(block(g, 2, 0), b1_sem.at[g, 2])
        to_second(g, 3)

    def b_second(g, j, d):
        ref = block(g, NEAR[j], 2 * d - 1)
        arrived(ref, b2_sem.at[g, j, d])
        go(ref.at[d], ref.at[d], b2_sem.at[g, j, 2], second(g, 1 - 2 * d), 1)
        to_sibling(g, j, 1 + d)

    def b_last(g, j):
        arrived(block(g, NEAR[j], 2), b2_sem.at[g, j, 2])
        to_sibling(g, j, 3)

    def b_sibling(g):
        arrived(b.at[0:16], bs_sem.at[g])

    def compute(p, g, low, high):
        base, r = PARTS[p]
        here = pl.ds(base, r)
        if low == 0:
            acc[2 * g : 2 * g + 2, pl.ds(2 * base, 2 * r), :] = jnp.zeros((2, 2 * r, 2 * W), jnp.float32)

        def body(m, carry):
            place = plane(((m + 1) // 2) * (2 * (m % 2) - 1))
            lhs = [a[side * 8 + place, :, here, :].reshape(2 * r, W) for side in (0, 1)]
            for n in range(2):
                which = xl if n == 0 else 1 - xl
                for cd in range(2):
                    total = acc[g * 2 + n, pl.ds(2 * base, 2 * r), cd * W : (cd + 1) * W]
                    for side in (0, 1):
                        total = total + jnp.dot(
                            lhs[side], b[(g * 16 + side * 8 + place) * 2 + which, cd],
                            preferred_element_type=jnp.float32)
                    acc[g * 2 + n, pl.ds(2 * base, 2 * r), cd * W : (cd + 1) * W] = total
            return carry

        lax.fori_loop(low, high, body, 0, unroll=high - low)

    def out_rows(p, half, quarter):
        base, r = PARTS[p]
        return out.at[:, pl.ds(base + half * HALF + quarter * QUARTER, r), :]

    def result(n, p):
        base, r = PARTS[p]
        return cs.at[n, :, pl.ds(base, r), :]

    AWAY = ((3, across), (2, outer), (1, partner))

    def finish(p, g):
        base, r = PARTS[p]
        here = pl.ds(base, r)
        for n in (2 * g + 1, 2 * g):
            top, low = pl.ds(2 * base, r), pl.ds(2 * base + r, r)
            dst = out_rows(p, xl, kind) if n == 0 else result(n, p)
            dst[0] = (acc[n, top, :W] - acc[n, low, W:]).astype(jnp.bfloat16)
            dst[1] = (acc[n, top, W:] + acc[n, low, :W]).astype(jnp.bfloat16)
        for n, where in AWAY:
            if n // 2 == g:
                go(result(n, p), out_rows(p, xl, kind), c_sem, where)

    barrier = pltpu.get_barrier_semaphore()
    for where in (at_x(1), at_x(-1), at_y(1), at_y(-1), inner, outer, across, sibling):
        pl.semaphore_signal(barrier, inc=1, device_id=where, device_id_type=MESH)
    for i in range(N):
        load(i, 0).start()
        load(i, 1).start()
        load(i, 2).start()
        load(i, 3).start()
        if i == 0:
            load_rot.start()
    pl.semaphore_wait(barrier, 8)

    b_out()
    b_start(0)
    swap(0)
    own(0, 0)
    swap(1)
    swap(2)
    own(1, 0)
    pass_on(0, 0, 5, 2)
    own(2, 0)
    b_start(1)
    b_second(0, 0, 0)
    b_second(0, 0, 1)
    b_first(0, 0)
    b_first(0, 1)
    pass_on(1, 0, 5, 2)
    pass_on(0, 0, 1, 6)
    pass_on(0, 0, 0, 7)
    pass_on(2, 0, 5, 2)
    own(0, 1)
    pass_on(1, 0, 1, 6)
    b_first(1, 0)
    b_first(1, 1)
    pass_on(0, 0, 6, 3)
    pass_on(1, 0, 0, 7)
    pass_on(0, 0, 2, 8)
    b_last(0, 0)
    pass_on(2, 0, 1, 6)
    pass_on(0, 1, 5, 2)
    pass_on(2, 0, 0, 7)
    pass_on(1, 0, 2, 8)
    b_second(0, 1, 0)
    b_second(0, 1, 1)
    pass_on(1, 0, 6, 3)
    pass_on(2, 0, 2, 8)
    b_second(1, 0, 0)
    b_second(1, 0, 1)
    pass_on(0, 1, 1, 6)
    b_far(0)
    pass_on(0, 1, 0, 7)
    b_second(0, 2, 0)
    b_second(0, 2, 1)
    pass_on(2, 0, 6, 3)
    pass_on(0, 0, 3, 9)
    b_far(1)
    pass_on(0, 1, 2, 8)
    b_second(1, 1, 0)
    b_second(1, 1, 1)
    pass_on(1, 0, 3, 9)
    b_last(0, 1)
    pass_on(2, 0, 3, 9)
    pass_on(0, 1, 6, 3)
    b_second(1, 2, 0)
    b_second(1, 2, 1)
    b_second(0, 3, 0)
    b_second(0, 3, 1)
    pass_on(0, 1, 3, 9)
    b_last(1, 0)
    b_last(0, 2)
    own(1, 1)
    b_last(0, 3)
    b_second(1, 3, 0)
    b_second(1, 3, 1)
    b_sibling(0)
    settle(0, 4)
    compute(0, 0, 0, 4)
    pass_on(1, 1, 1, 6)
    settle(0, 8)
    compute(0, 0, 4, 7)
    settle(0, 9)
    compute(0, 0, 7, 8)
    finish(0, 0)
    b_last(1, 1)
    pass_on(1, 1, 5, 2)
    own(2, 1)
    pass_on(1, 1, 0, 7)
    b_last(1, 2)
    pass_on(1, 1, 6, 3)
    pass_on(1, 1, 2, 8)
    b_last(1, 3)
    pass_on(2, 1, 5, 2)
    pass_on(2, 1, 1, 6)
    b_sibling(1)
    compute(0, 1, 0, 4)
    pass_on(2, 1, 0, 7)
    compute(0, 1, 4, 7)
    compute(0, 1, 7, 8)
    finish(0, 1)
    settle(1, 4)
    compute(1, 1, 0, 4)
    pass_on(1, 1, 3, 9)
    compute(1, 0, 0, 4)
    pass_on(2, 1, 2, 8)
    settle(1, 8)
    compute(1, 1, 4, 7)
    compute(1, 0, 4, 7)
    pass_on(2, 1, 6, 3)
    settle(2, 4)
    compute(2, 1, 0, 4)
    compute(2, 0, 0, 4)
    settle(1, 9)
    compute(1, 1, 7, 8)
    finish(1, 1)
    pass_on(2, 1, 3, 9)
    compute(1, 0, 7, 8)
    finish(1, 0)
    settle(2, 8)
    compute(2, 1, 4, 7)
    compute(2, 0, 4, 7)
    settle(2, 9)
    compute(2, 1, 7, 8)
    finish(2, 1)
    compute(2, 0, 7, 8)
    finish(2, 0)

    remote(b.at[0:32], b.at[0:32], send_sem.at[0], c_sem, sibling).wait_send()
    remote(b.at[0:56], b.at[0:56], send_sem.at[1], c_sem, sibling).wait_send()
    arrived(cs.at[0:3], c_sem)


def local(waves, rotation):
    dma = pltpu.SemaphoreType.DMA
    bf16 = jnp.bfloat16
    return pl.pallas_call(
        kernel,
        out_shape=pltpu.VMEM(waves.shape, waves.dtype),
        in_specs=[pl.BlockSpec(memory_space=pl.ANY)] * 2,
        out_specs=pl.BlockSpec(memory_space=pltpu.VMEM),
        scratch_shapes=[
            pltpu.VMEM((16, 2, QUARTER, W), bf16),
            pltpu.VMEM((2, 2, QUARTER, W), bf16),
            pltpu.VMEM((3, 2, 2, QUARTER, W), bf16),
            pltpu.VMEM((2, 2, QUARTER, W), bf16),
            pltpu.VMEM((64, 2, W, W), bf16),
            pltpu.VMEM((4, 2, QUARTER, W), bf16),
            pltpu.VMEM((4, 2 * QUARTER, 2 * W), jnp.float32),
            dma((2, N + 1)), dma((2,)), dma((N,)), dma((N, 15)), dma,
            dma((2, 3)), dma((2, 4, 3)), dma((2,)), dma,
        ],
        compiler_params=pltpu.CompilerParams(
            collective_id=0, has_side_effects=True, vmem_limit_bytes=60 * 1024 * 1024),
        name="rotate",
    )(waves, rotation)


def solution(mesh):
    finer = Mesh(
        mesh.devices.reshape(2, 4, 2, 2, 8), ("xh", "y", "core", "xl", "z")
    )
    return jax.shard_map(
        local,
        mesh=finer,
        in_specs=(P(None, GA, BAND), P(None, GA, BAND)),
        out_specs=P(None, GA, BAND),
        check_vma=False,
    )
```
